32 devices in a mesh: seq: 8 (over z, core), vocab: 4 (over y, x).
Axes of the slice: x: 2, y: 2, z: 4, core: 2. Of those that a mesh axis runs over, the one named last changes fastest.
Arguments:
- probe_states: bfloat16 [3, 8192, 6144], P(None, 'seq', 'vocab'), may hold values from -6 to 6
- final_states: bfloat16 [8192, 6144], P('seq', 'vocab'), may hold values from -6 to 6
- translator: bfloat16 [3, 6144, 6144], P(None, 'vocab', 'seq'), may hold values from -0.078125 to 0.078125
- translator_bias: float32 [3, 6144], P(None, 'seq'), may hold values from -4 to 4
- norm_gain: float32 [6144], P('seq'), may hold values from 0.5 to 1.5
- unembed: bfloat16 [32768, 6144], P('vocab', 'seq'), may hold values from -0.21875 to 0.21875
- answer_rows: int32 [8, 32], P('seq'), may hold values from 0 to 1023, as said below
- answer_count: int32 [8], P('seq'), may hold values from 1 to 32, 128 in all
- targets: int32 [8, 32], P('seq'), may hold values from 0 to 32767
Outputs:
- answer_logprob: float32 [4, 8, 32], P(None, 'seq')
- answer_kl: float32 [3, 8, 32], P(None, 'seq')
The draws below stay inside these ranges and needn't reach their ends.
Inputs may be any that keep to these rules, and one draw needn't show every extreme that they name: `answer_rows`: each row holds 32 different positions. `answer_count`: the counts sum to 128, and some sequence has 32.
All inputs are finite; a program needn't handle non-finite values. No bound on the sum of `answer_count` on one device may be relied on, other than what follows from the above.
Results may differ from the reference program's by a relative error of at most 0.00099.
Values may be sent and summed in bfloat16 or wider, within the bound.
A program may use at most 128 MiB of HBM per device.

```python
import math
import jax
import jax.numpy as jnp
import numpy as np
from jax import lax

D = 6144
V = 32768
LAYERS = 3
LENGTH = 1024
CAP = 32
SEQS = 8
TOKENS = 8192
FLAGGED = 128


def draw_answer_rows(key, part):
    seqs = TOKENS // LENGTH
    scores = jax.random.randint(key, (seqs, LENGTH), 0, 1 << 20)
    scores = scores * LENGTH + jnp.arange(LENGTH, dtype=jnp.int32)[None, :]
    order = jnp.argsort(scores, axis=1)
    return order[:, :CAP].astype(jnp.int32)


def place_ends(drawn, stream_key, least, high):
    spot = [jax.random.randint(jax.random.fold_in(stream_key, axis), (), 0, length) for axis, length in enumerate(drawn.shape)]
    widest = drawn.shape.index(max(drawn.shape))
    neighbour = spot[:widest] + [(spot[widest] + 1) % drawn.shape[widest]] + spot[widest + 1:]
    return drawn.at[tuple(spot)].set(least).at[tuple(neighbour)].set(high)


def block_scale(key, extent, shards, least, largest):
    def one(dim, blocks):
        heights = jax.random.uniform(jax.random.fold_in(jax.random.fold_in(key, 6), dim), (blocks,), jnp.float32, least / len(shards), largest / len(shards))
        return jnp.repeat(jnp.exp(heights), extent[dim] // blocks).reshape((-1,) + (1,) * (len(extent) - dim - 1))

    gain = one(*shards[0])
    for cut in shards[1:]:
        gain = gain * one(*cut)
    return gain


def rank_table(number_of, lean):
    weights = [(1 << 20) // math.isqrt(standing ** lean) + 1 for standing in range(1, number_of + 1)]
    scale = 1 + sum(weights) // (1 << 30)
    return np.cumsum(np.array([max(1, weight // scale) for weight in weights]))


def ranked(stream_key, extent, number_of, lean):
    grid = rank_table(number_of, lean)
    ticket = jax.random.randint(jax.random.fold_in(stream_key, 1), extent, 0, int(grid[number_of - 1]))
    rank = jnp.searchsorted(jnp.asarray(grid, jnp.int32), ticket, side="right")
    return jax.random.permutation(jax.random.fold_in(stream_key, 2), number_of)[rank].astype(jnp.int32)


def length_profile(count, total, bound, skew):
    weights = [(1 << 20) // math.isqrt(rank ** skew) + 1 for rank in range(2, count + 1)]
    rest, counts = total - bound - (count - 1), [1] * (count - 1)
    while rest > 0:
        free = [i for i in range(count - 1) if counts[i] < bound]
        mass, budget = sum([weights[i] for i in free]), rest
        for i in free:
            extra = min(bound - counts[i], max(1, budget * weights[i] // mass), rest)
            counts[i] = counts[i] + extra
            rest = rest - extra
    return np.array([bound] + counts)


def ragged_sizes(key, amount, total, most, lean):
    if amount == 2:
        one = jax.random.randint(key, (), max(1, total - most), min(most, total - 1) + 1)
        return jnp.stack([one, total - one])
    tallies = jnp.asarray(length_profile(amount, total, most, lean), jnp.int32)
    twos = (amount - 1) // 2
    giver, receiver = tallies[1:1 + 2 * twos:2], tallies[2:2 + 2 * twos:2]
    room = jnp.minimum(giver - 1, most - receiver)
    shifted = jax.random.randint(jax.random.fold_in(key, 1), (twos,), 0, 1 << 20) % (room + 1)
    tallies = tallies.at[1:1 + 2 * twos:2].set(giver - shifted).at[2:2 + 2 * twos:2].set(receiver + shifted)
    return tallies[jax.random.permutation(jax.random.fold_in(key, 2), amount)]


def gaussian(own_key, dims, deviation, reach, split=(), kind=jnp.bfloat16):
    result = deviation * jax.random.normal(own_key, dims, jnp.float32)
    if split:
        result = result * block_scale(own_key, dims, split, -0.22, 0.18)
    return jnp.clip(result, -reach, reach).astype(kind)


def setup_inputs(seed: int = 0) -> dict:
    key_of = jax.random.split(jax.random.key(seed), 10)
    probe_states = gaussian(key_of[0], (LAYERS, TOKENS, D), 1.0, 6.0, ((1, 8), (2, 4)))
    final_states = gaussian(key_of[1], (TOKENS, D), 1.0, 6.0, ((0, 8), (1, 4)))
    translator = gaussian(key_of[2], (LAYERS, D, D), D ** -0.5, 0.078125, ((1, 4), (2, 8)))
    translator_bias = gaussian(key_of[3], (LAYERS, D), 0.5, 4.0, ((1, 8),), jnp.float32)
    norm_gain = jnp.clip(1.0 + 0.1 * jax.random.normal(key_of[4], (D,), jnp.float32), 0.5, 1.5)
    unembed = gaussian(key_of[5], (V, D), (D // 9) ** -0.5, 0.21875, ((0, 4), (1, 8)))
    answer_rows = draw_answer_rows(jax.random.fold_in(key_of[9], 71), 0)
    answer_count = ragged_sizes(key_of[7], SEQS, FLAGGED, CAP, 2).astype(jnp.int32)
    targets = place_ends(ranked(key_of[8], (SEQS, CAP), V, 2), jax.random.fold_in(key_of[8], 3), 0, V - 1).astype(jnp.int32)
    return {"probe_states": probe_states, "final_states": final_states, "translator": translator, "translator_bias": translator_bias, "norm_gain": norm_gain, "unembed": unembed, "answer_rows": answer_rows, "answer_count": answer_count, "targets": targets}


def lens_logits(rows, norm_gain, unembed_f):
    mean_sq = lax.optimization_barrier(jnp.mean(rows * rows, axis=-1))
    scaled = (rows * norm_gain).astype(jnp.bfloat16)
    raw = jnp.dot(scaled.astype(jnp.float32), unembed_f.T, precision=lax.Precision.HIGHEST)
    return raw * lax.rsqrt(mean_sq + 1e-05)[:, None]

def reference(probe_states, final_states, translator, translator_bias, norm_gain, unembed, answer_rows, answer_count, targets):
    seqs = answer_rows.shape[0]
    flat = (jnp.arange(seqs, dtype=jnp.int32)[:, None] * LENGTH + answer_rows.astype(jnp.int32)).reshape(-1)
    live = (jnp.arange(CAP, dtype=jnp.int32)[None, :] < answer_count[:, None]).reshape(-1)
    wanted = targets.reshape(-1)[:, None]
    unembed_f = unembed.astype(jnp.float32)
    final_rows = jnp.take(final_states, flat, axis=0).astype(jnp.float32)
    final_logits = lens_logits(final_rows, norm_gain, unembed_f)
    final_lse = jnp.log(lax.optimization_barrier(jnp.sum(jnp.exp(final_logits), axis=-1)))
    final_prob = jnp.exp(final_logits - final_lse[:, None])
    logprobs = []
    divergences = []
    for layer in range(LAYERS):
        rows = jnp.take(probe_states[layer], flat, axis=0)
        lensed = rows.astype(jnp.float32) + jnp.dot(rows.astype(jnp.float32), translator[layer].astype(jnp.float32), precision=lax.Precision.HIGHEST) + translator_bias[layer]
        logits = lens_logits(lensed, norm_gain, unembed_f)
        lse = jnp.log(lax.optimization_barrier(jnp.sum(jnp.exp(logits), axis=-1)))
        logprobs.append(jnp.take_along_axis(logits, wanted, axis=1)[:, 0] - lse)
        divergences.append(lax.optimization_barrier(jnp.sum(final_prob * (final_logits - logits), axis=-1)) - final_lse + lse)
    logprobs.append(jnp.take_along_axis(final_logits, wanted, axis=1)[:, 0] - final_lse)
    logprob = jnp.where(live[None, :], jnp.stack(logprobs), 0.0).reshape(LAYERS + 1, seqs, CAP)
    divergence = jnp.where(live[None, :], jnp.stack(divergences), 0.0).reshape(LAYERS, seqs, CAP)
    return (logprob, divergence)
```

```python
import math
import jax
import jax.numpy as jnp
from jax import lax
from jax.sharding import PartitionSpec as P

FLAG_DEV = 16
STATE_MAX, MATRIX_MAX, BIAS_MAX, GAIN_MAX, UNEMBED_MAX = 6.0, 0.078125, 4.0, 1.5, 0.21875


def line_scatter(weight, scaled, shrink, seq_count, seq_index):
    f32, f16 = jnp.float32, jnp.float16
    chips = seq_count // 2
    chip, core = seq_index // 2, seq_index % 2
    own = weight.shape[0] // seq_count
    swap = [(s, s + 1 - 2 * (s % 2)) for s in range(seq_count)]
    up = [(s, s + 2) for s in range(seq_count - 2)]
    down = [(s + 2, s) for s in range(seq_count - 2)]

    def partial(owner):
        block = lax.dynamic_slice_in_dim(weight, owner * own, own, axis=0)
        dims = (((1,), (1,)), ((), ()))
        return lax.dot_general(block, scaled, dims, preferred_element_type=f32) * shrink

    def held(target):
        other = lax.ppermute(partial(target * 2 + 1 - core).astype(f16), "seq", swap)
        return partial(target * 2 + core) + other.astype(f32)

    rise = fall = None
    for step in range(chips - 1):
        send_up = held(jnp.minimum(chips - 1 - step + chip, chips - 1))
        send_down = held(jnp.maximum(chip - (chips - 1 - step), 0))
        if step:
            send_up = send_up + rise.astype(f32)
            send_down = send_down + fall.astype(f32)
        rise = lax.ppermute(send_up.astype(f16), "seq", up)
        fall = lax.ppermute(send_down.astype(f16), "seq", down)
    return held(chip) + (rise.astype(f32) + fall.astype(f32))


def body(
    probe_states,
    final_states,
    translator,
    translator_bias,
    norm_gain,
    unembed,
    answer_rows,
    answer_count,
    targets,
):
    f32 = jnp.float32
    bf16 = jnp.bfloat16
    seq_count = lax.axis_size("seq")
    vocab_count = lax.axis_size("vocab")
    seq_index = lax.axis_index("seq")
    vocab_index = lax.axis_index("vocab")
    layers = probe_states.shape[0]
    cap = answer_rows.shape[1]
    width_in = probe_states.shape[2]
    width_out = translator.shape[2]
    vocab_part = unembed.shape[0]
    model = width_in * vocab_count
    total = seq_count * FLAG_DEV
    stacked = (layers + 1) * total
    picks = answer_rows[0]

    probed = jnp.take(probe_states, picks, axis=1, mode="clip")
    local = jnp.concatenate(
        [probed[l] for l in range(layers)] + [jnp.take(final_states, picks, axis=0, mode="clip")],
        axis=1,
    )
    gathered = lax.all_gather(local, "seq", axis=0, tiled=True)
    meta = lax.all_gather(
        jnp.concatenate([answer_count[None, :], targets], axis=1), "seq", axis=0, tiled=True
    )
    counts, targets_all = meta[:, 0], meta[:, 1:]
    order = jnp.arange(seq_count, dtype=jnp.int32)
    starts = jnp.sum(jnp.where(order[:, None] < order[None, :], counts[:, None], 0), axis=0)
    slots = jnp.arange(cap, dtype=jnp.int32)
    place = jnp.where(slots[None, :] < counts[:, None], starts[:, None] + slots[None, :], -1)
    hit = place.reshape(-1)[None, :] == jnp.arange(total, dtype=jnp.int32)[:, None]
    row_targets = jnp.sum(jnp.where(hit, targets_all.reshape(-1)[None, :], 0), axis=1)

    rows = jnp.dot(hit.astype(bf16), gathered, preferred_element_type=f32).astype(bf16)
    parts = [rows[:, l * width_in : (l + 1) * width_in] for l in range(layers + 1)]
    in_pos = vocab_index * width_in + jnp.arange(width_in, dtype=jnp.int32)
    out_pos = seq_index * width_out + jnp.arange(width_out, dtype=jnp.int32)
    identity = (in_pos[:, None] == out_pos[None, :]).astype(bf16)
    bias = jnp.where(vocab_index == 0, translator_bias, 0.0)
    pieces = []
    for l in range(layers + 1):
        piece = jnp.dot(parts[l], identity, preferred_element_type=f32)
        if l < layers:
            piece = piece + jnp.dot(parts[l], translator[l], preferred_element_type=f32) + bias[l]
        pieces.append(piece)
    partial_value = jnp.concatenate(pieces, axis=0)
    lensed = lax.psum_scatter(partial_value, "vocab", scatter_dimension=0, tiled=True)
    squares = jnp.sum(lensed * lensed, axis=1)
    scaled = lax.all_gather(
        (lensed * norm_gain[None, :]).astype(bf16), "vocab", axis=0, tiled=True
    )
    chunk = stacked // vocab_count
    spread = jnp.where(
        jnp.arange(vocab_count, dtype=jnp.int32)[:, None] == vocab_index,
        squares.reshape(1, chunk),
        0.0,
    )
    every_square = lax.psum(lax.psum(spread, "vocab"), "seq").reshape(stacked)
    factor = lax.rsqrt(every_square / model + 1e-05)

    widest = GAIN_MAX * UNEMBED_MAX * model * (STATE_MAX + BIAS_MAX + model * STATE_MAX * MATRIX_MAX)
    shrink = 2.0 ** -max(0, math.ceil(math.log2(widest / 60000.0)))
    term = line_scatter(unembed, scaled, shrink, seq_count, seq_index)
    logits = term * (factor / shrink)[None, :]
    own_vocab = vocab_part // seq_count
    expz = jnp.exp(logits)
    total_exp = jnp.sum(expz, axis=0).reshape(layers + 1, total)
    final = slice(layers * total, stacked)
    cross = jnp.stack(
        [
            jnp.sum(
                expz[:, final] * (logits[:, final] - logits[:, l * total : (l + 1) * total]), axis=0
            )
            for l in range(layers)
        ]
    )
    ids = row_targets - (vocab_index * vocab_part + seq_index * own_vocab)
    target_hit = jnp.arange(own_vocab, dtype=jnp.int32)[:, None] == jnp.tile(ids, layers + 1)[None, :]
    picked = jnp.sum(jnp.where(target_hit, logits, 0.0), axis=0).reshape(layers + 1, total)
    sums = lax.psum(lax.psum(jnp.concatenate([total_exp, cross, picked], axis=0), "vocab"), "seq")
    total_exp = sums[: layers + 1]
    cross = sums[layers + 1 : 2 * layers + 1]
    picked = sums[2 * layers + 1 :]
    log_total = jnp.log(total_exp)
    logprob = picked - log_total
    divergence = cross / total_exp[layers:] - log_total[layers:] + log_total[:layers]
    results = jnp.concatenate([logprob, divergence], axis=0)
    mine = lax.dynamic_slice_in_dim(place, seq_index, 1, axis=0)
    own = mine.reshape(cap, 1) == jnp.arange(total, dtype=jnp.int32)[None, :]
    out = jnp.sum(jnp.where(own[None], results[:, None, :], 0.0), axis=2)
    return (out[: layers + 1, None, :], out[layers + 1 :, None, :])


def solution(mesh):
    in_specs = (
        P(None, "seq", "vocab"),
        P("seq", "vocab"),
        P(None, "vocab", "seq"),
        P(None, "seq"),
        P("seq"),
        P("vocab", "seq"),
        P("seq", None),
        P("seq"),
        P("seq", None),
    )
    out_specs = (P(None, "seq", None), P(None, "seq", None))
    return jax.shard_map(body, mesh=mesh, in_specs=in_specs, out_specs=out_specs, check_vma=False)
```
